128 devices in a mesh: tp: 4 (over x), dp: 32 (over z, y, core).
Axes of the slice: x: 4, y: 4, z: 4, core: 2. Of those that a mesh axis runs over, the one named last changes fastest.
Arguments:
- hidden: bfloat16 [32, 256, 7168], P('dp', 'tp')
- norm_gain: bfloat16 [7168], P('dp')
- w_query: bfloat16 [7168, 7168], P('dp', 'tp')
- w_key: bfloat16 [7168, 1024], P('dp', 'tp')
- w_value: bfloat16 [7168, 1024], P('dp', 'tp')
- w_out: bfloat16 [7168, 7168], P('tp', 'dp')
- grad_out: bfloat16 [32, 256, 7168], P('dp', 'tp')
Outputs:
- output 1: bfloat16 [32, 256, 7168], P('dp', 'tp')
- output 2: bfloat16 [32, 256, 7168], P('dp', 'tp')
- output 3: float32 [7168], P('dp')
- output 4: float32 [7168, 7168], P('dp', 'tp')
- output 5: float32 [7168, 1024], P('dp', 'tp')
- output 6: float32 [7168, 1024], P('dp', 'tp')
- output 7: float32 [7168, 7168], P('tp', 'dp')
All inputs are finite; a program needn't handle non-finite values.
Results may differ from the reference program's by a relative error of at most 0.0184718.
Values are sent between devices in bfloat16 or wider.
A program may use at most 1 GiB of HBM per device.

```python
import jax
import jax.numpy as jnp
from jax import lax

BATCH_SIZE = 32
SEQ_LEN = 256
MODEL_DIM = 7168
NUM_HEADS = 56
NUM_KV = 8
HEAD_DIM = 128
NORM_EPS = 1e-5
ROPE_BASE = 500000.0
GROUP_SIZE = NUM_HEADS // NUM_KV
SCORE_SCALE = HEAD_DIM ** -0.5


def setup_inputs(seed: int = 0) -> dict:
    key_list = jax.random.split(jax.random.key(seed), 7)
    q_width = NUM_HEADS * HEAD_DIM
    kv_width = NUM_KV * HEAD_DIM
    act_shape = (BATCH_SIZE, SEQ_LEN, MODEL_DIM)
    in_scale = MODEL_DIM ** -0.5
    hidden = jax.random.normal(key_list[0], act_shape, jnp.float32)
    norm_gain = 1.0 + 0.3 * jax.random.normal(key_list[1], (MODEL_DIM,), jnp.float32)
    w_query = (1.25 * in_scale) * jax.random.normal(key_list[2], (MODEL_DIM, q_width), jnp.float32)
    w_key = (1.25 * in_scale) * jax.random.normal(key_list[3], (MODEL_DIM, kv_width), jnp.float32)
    w_value = in_scale * jax.random.normal(key_list[4], (MODEL_DIM, kv_width), jnp.float32)
    w_out = (2.0 * q_width ** -0.5) * jax.random.normal(key_list[5], (q_width, MODEL_DIM), jnp.float32)
    grad_out = jax.random.normal(key_list[6], act_shape, jnp.float32)
    return {
        "hidden": hidden.astype(jnp.bfloat16),
        "norm_gain": norm_gain.astype(jnp.bfloat16),
        "w_query": w_query.astype(jnp.bfloat16),
        "w_key": w_key.astype(jnp.bfloat16),
        "w_value": w_value.astype(jnp.bfloat16),
        "w_out": w_out.astype(jnp.bfloat16),
        "grad_out": grad_out.astype(jnp.bfloat16),
    }


def rope_tables():
    half_dim = HEAD_DIM // 2
    inv_freq = ROPE_BASE ** (-jnp.arange(half_dim, dtype=jnp.float32) * 2.0 / HEAD_DIM)
    angles = jnp.arange(SEQ_LEN, dtype=jnp.float32)[:, None] * inv_freq[None, :]
    return jnp.cos(angles), jnp.sin(angles)


def rotate(values, cos_t, sin_t):
    half_dim = values.shape[-1] // 2
    lower_half = values[..., :half_dim]
    upper_half = values[..., half_dim:]
    return jnp.concatenate([lower_half * cos_t - upper_half * sin_t, upper_half * cos_t + lower_half * sin_t], axis=-1)


def to_bf16(values):
    return values.astype(jnp.bfloat16).astype(jnp.float32)


def group_attention(items):
    q_blk, k_blk, v_blk = items
    scores = jnp.einsum("qrd,kd->rqk", q_blk, k_blk) * SCORE_SCALE
    causal = jnp.arange(SEQ_LEN)[:, None] >= jnp.arange(SEQ_LEN)[None, :]
    scores = jnp.where(causal[None], scores, -1e30)
    attn_prob = to_bf16(jax.nn.softmax(scores, axis=-1))
    return to_bf16(jnp.einsum("rqk,kd->qrd", attn_prob, v_blk))


def block_forward(hidden, norm_gain, w_query, w_key, w_value, w_out):
    cos_t, sin_t = rope_tables()
    inv_rms = lax.rsqrt(jnp.mean(hidden * hidden, axis=-1, keepdims=True) + NORM_EPS)
    normed = to_bf16(hidden * inv_rms * norm_gain).reshape(-1, MODEL_DIM)
    q_lin = to_bf16(jnp.dot(normed, w_query, preferred_element_type=jnp.float32))
    k_lin = to_bf16(jnp.dot(normed, w_key, preferred_element_type=jnp.float32))
    v_lin = to_bf16(jnp.dot(normed, w_value, preferred_element_type=jnp.float32))
    q_heads = to_bf16(rotate(q_lin.reshape(BATCH_SIZE, SEQ_LEN, NUM_KV, GROUP_SIZE, HEAD_DIM), cos_t[:, None, None, :], sin_t[:, None, None, :]))
    k_heads = to_bf16(rotate(k_lin.reshape(BATCH_SIZE, SEQ_LEN, NUM_KV, HEAD_DIM), cos_t[:, None, :], sin_t[:, None, :]))
    v_heads = v_lin.reshape(BATCH_SIZE, SEQ_LEN, NUM_KV, HEAD_DIM)
    q_items = jnp.moveaxis(q_heads, 2, 1).reshape(BATCH_SIZE * NUM_KV, SEQ_LEN, GROUP_SIZE, HEAD_DIM)
    k_items = jnp.moveaxis(k_heads, 2, 1).reshape(BATCH_SIZE * NUM_KV, SEQ_LEN, HEAD_DIM)
    v_items = jnp.moveaxis(v_heads, 2, 1).reshape(BATCH_SIZE * NUM_KV, SEQ_LEN, HEAD_DIM)
    attn_items = lax.map(jax.checkpoint(group_attention), (q_items, k_items, v_items))
    attn_out = jnp.moveaxis(attn_items.reshape(BATCH_SIZE, NUM_KV, SEQ_LEN, GROUP_SIZE, HEAD_DIM), 1, 2).reshape(BATCH_SIZE * SEQ_LEN, NUM_HEADS * HEAD_DIM)
    block_out = to_bf16(jnp.dot(attn_out, w_out, preferred_element_type=jnp.float32))
    return hidden + block_out.reshape(BATCH_SIZE, SEQ_LEN, MODEL_DIM)


def reference(hidden, norm_gain, w_query, w_key, w_value, w_out, grad_out):
    out_f32, pullback = jax.vjp(
        block_forward,
        hidden.astype(jnp.float32),
        norm_gain.astype(jnp.float32),
        w_query.astype(jnp.float32),
        w_key.astype(jnp.float32),
        w_value.astype(jnp.float32),
        w_out.astype(jnp.float32),
    )
    grad_list = pullback(grad_out.astype(jnp.float32))
    return (
        out_f32.astype(jnp.bfloat16),
        grad_list[0].astype(jnp.bfloat16),
        grad_list[1],
        grad_list[2],
        grad_list[3],
        grad_list[4],
        grad_list[5],
    )
```

```python
import functools

import jax
import jax.numpy as jnp
from jax import lax
from jax.experimental import pallas as pl
from jax.experimental.pallas import tpu as pltpu
from jax.sharding import PartitionSpec as P

HEAD_DIM = 128
NORM_EPS = 1e-5
ROPE_BASE = 500000.0
SCORE_SCALE = HEAD_DIM ** -0.5
MASK_VALUE = -1e30
MESH = pl.DeviceIdType.MESH
ANY = pl.BlockSpec(memory_space=pl.ANY)
VMEM = pl.BlockSpec(memory_space=pltpu.VMEM)
F32, BF16 = jnp.float32, jnp.bfloat16

D = 7168
SEQ = 256
POS = 64
BLK = 448
HALF = 224
DZ = 1792
W_COLS = (640, 512, 384, 512)
Z_FIRST = (True, False, True, False)


class Place:
    def __init__(self):
        self.x = lax.axis_index("tp")
        dp = lax.axis_index("dp")
        self.z, self.y, self.c = dp // 8, (dp // 2) % 4, dp % 2

    def at(self, x=0, y=0, z=0, c=0):
        x, y, z = (self.x + x + 4) % 4, (self.y + y + 4) % 4, (self.z + z + 4) % 4
        return (x, (z * 4 + y) * 2 + (self.c + c) % 2)


def enter(place, offsets):
    barrier = pltpu.get_barrier_semaphore()
    for off in offsets:
        pl.semaphore_signal(barrier, inc=1, device_id=place.at(**off), device_id_type=MESH)
    pl.semaphore_wait(barrier, len(offsets))


def around(axis):
    return [{axis: 1}, {axis: -1}, {axis: 2}]


class Copies:
    def __init__(self, send, recv):
        self.send, self.recv, self.n, self.all = send, recv, 0, []

    def remote(self, src, dst, device):
        cp = pltpu.make_async_remote_copy(src, dst, self.send.at[self.n], self.recv.at[self.n], device_id=device, device_id_type=MESH)
        self.n += 1
        cp.start()
        self.all.append(cp)
        return cp

    def local(self, src, dst):
        cp = pltpu.make_async_copy(src, dst, self.send.at[self.n])
        self.n += 1
        cp.start()
        return cp

    def drain(self):
        for cp in self.all:
            cp.wait_send()


class Ring:
    def __init__(self, copies, place, axis, piece, own=None):
        self.copies, self.piece = copies, piece
        self.right, self.left = place.at(**{axis: 1}), place.at(**{axis: -1})
        self.own = own or (lambda h: piece(0, h))

    def start(self):
        c, p = self.copies, self.piece
        self.r0 = c.remote(self.own(0), p(0, 0), self.right)
        self.l0 = c.remote(self.own(1), p(0, 1), self.left)
        self.r1 = c.remote(self.own(1), p(0, 1), self.right)
        self.l1 = c.remote(self.own(0), p(0, 0), self.left)

    def forward(self):
        c, p = self.copies, self.piece
        self.r0.wait_recv()
        self.r2 = c.remote(p(-1, 0), p(-1, 0), self.right)
        self.l0.wait_recv()
        self.l2 = c.remote(p(1, 1), p(1, 1), self.left)

    def near(self):
        self.r1.wait_recv()
        self.l1.wait_recv()

    def far(self):
        self.r2.wait_recv()
        self.l2.wait_recv()


def params(cid, vmem=None):
    return pltpu.CompilerParams(collective_id=cid, has_side_effects=True, vmem_limit_bytes=vmem)


def gain_kernel(g_ref, o_ref, send, recv):
    me = Place()
    enter(me, [{"c": 1}] + around("y") + around("z"))
    cs = Copies(send, recv)
    o_ref[me.z, me.y, me.c] = g_ref[...]
    cs.remote(g_ref, o_ref.at[me.z, me.y, me.c], me.at(c=1)).wait_recv()
    for cp in [cs.remote(o_ref.at[me.z, me.y], o_ref.at[me.z, me.y], me.at(**off)) for off in around("y")]:
        cp.wait_recv()
    for cp in [cs.remote(o_ref.at[me.z], o_ref.at[me.z], me.at(**off)) for off in around("z")]:
        cp.wait_recv()
    cs.drain()


def gather_gain(norm_gain):
    padded = jnp.pad(norm_gain.astype(F32), (0, 1024 - HALF)).reshape(8, 128)
    out = pl.pallas_call(
        gain_kernel,
        out_shape=jax.ShapeDtypeStruct((4, 4, 2, 8, 128), F32),
        in_specs=[VMEM], out_specs=VMEM,
        scratch_shapes=[pltpu.SemaphoreType.DMA((7,)), pltpu.SemaphoreType.DMA((7,))],
        compiler_params=params(0), name="gather_gain",
    )(padded)
    return out.reshape(32, 1024)[:, :HALF].reshape(D)


def gather_kernel(*refs):
    w_in, (n_in, dy_in, n4_in, dy4_in) = refs[:4], refs[4:8]
    w_all, (n_all, dy_all, n4_all, dy4_all) = refs[8:12], refs[12:16]
    send, recv = refs[16:]
    me = Place()
    enter(me, [{"c": 1}] + around("x") + around("y") + around("z"))
    cs = Copies(send, recv)
    mate = me.at(c=1)

    rows = pl.ds(pl.multiple_of(me.c * HALF, HALF), HALF)
    first = []
    for w, buf in zip(w_in, w_all):
        first.append((cs.remote(w.at[1 - me.c], buf.at[me.z, me.y, rows], mate), cs.local(w.at[me.c], buf.at[me.z, me.y, rows])))

    def x_piece(buf):
        return lambda off, h: buf.at[me.c, (me.x + off + 4) % 4, pl.ds(h * 32, 32)]

    def x_ring(buf, src):
        return Ring(cs, me, "x", x_piece(buf), lambda h: src.at[pl.ds(h * 32, 32)])

    def x4_ring(buf):
        return Ring(cs, me, "x", lambda off, h: buf.at[pl.ds(2 * h, 2), me.c, (me.x + off + 4) % 4])

    acts = []
    for buf, src in ((n_all, n_in), (dy_all, dy_in)):
        ring = x_ring(buf, src)
        ring.start()
        acts.append((ring, cs.local(src, buf.at[me.c, me.x]), buf))
    fours = []
    for buf, src, axis in ((n4_all, n4_in, "z"), (dy4_all, dy4_in, "y")):
        here = getattr(me, axis)
        moves = [cs.remote(src.at[(here + off[axis] + 4) % 4], buf.at[here, me.c, me.x], me.at(**off)) for off in around(axis)]
        fours.append((moves, cs.local(src.at[here], buf.at[here, me.c, me.x]), x4_ring(buf), buf))

    def phase1(buf, z_first):
        if z_first:
            return Ring(cs, me, "z", lambda off, h: buf.at[(me.z + off + 4) % 4, me.y, pl.ds(h * HALF, HALF)])
        return Ring(cs, me, "y", lambda off, h: buf.at[me.z, (me.y + off + 4) % 4, pl.ds(h * HALF, HALF)])

    def phase2(buf, z_first):
        if z_first:
            return Ring(cs, me, "y", lambda off, h: buf.at[pl.ds(2 * h, 2), (me.y + off + 4) % 4])
        return Ring(cs, me, "z", lambda off, h: buf.at[(me.z + off + 4) % 4, pl.ds(2 * h, 2)])

    ones = [phase1(b, f) for b, f in zip(w_all, Z_FIRST)]
    twos = [phase2(b, f) for b, f in zip(w_all, Z_FIRST)]
    for (remote, local), ring in zip(first, ones):
        remote.wait_recv()
        local.wait()
        ring.start()
    for ring in ones:
        ring.forward()
    for one, two in zip(ones[:2], twos[:2]):
        one.near()
        one.far()
        two.start()
    for one, two in zip(ones[2:], twos[2:]):
        one.near()
        one.far()
        two.start()
    for ring, local, buf in acts:
        local.wait()
        ring.forward()
        ring.near()
    for moves, local, ring, buf in fours:
        for cp in moves:
            cp.wait_recv()
        local.wait()
        ring.start()
    tail = []
    for ring, local, buf in acts:
        for k in (0, 1, -1):
            p = buf.at[me.c, (me.x + k + 4) % 4]
            tail.append(cs.remote(p, p, mate))
    for ring in twos[:2]:
        ring.forward()
    for ring, local, buf in acts:
        ring.far()
        p = buf.at[me.c, (me.x + 2) % 4]
        tail.append(cs.remote(p, p, mate))
    for moves, local, ring, buf in fours:
        ring.forward()
        ring.near()
        for k in (0, 1, -1):
            p = buf.at[:, me.c, (me.x + k + 4) % 4]
            tail.append(cs.remote(p, p, mate))
    for ring in twos[2:]:
        ring.forward()
    for moves, local, ring, buf in fours:
        ring.far()
        p = buf.at[:, me.c, (me.x + 2) % 4]
        tail.append(cs.remote(p, p, mate))
    for ring in twos:
        ring.near()
        ring.far()
    for cp in tail:
        cp.wait_recv()
    cs.drain()


def gather_all(w_in, normed, grad_out, normed4, grad4):
    n_cp = 4 * 14 + 2 * 7 + 2 * 10 + 16
    shapes = [jax.ShapeDtypeStruct((4, 4, BLK, cols), BF16) for cols in W_COLS]
    shapes += [jax.ShapeDtypeStruct((2, 4, POS, D), BF16)] * 2
    shapes += [jax.ShapeDtypeStruct((4, 2, 4, POS, DZ), BF16)] * 2
    return pl.pallas_call(
        gather_kernel,
        out_shape=shapes,
        in_specs=[VMEM] * 8, out_specs=[ANY] * 8,
        scratch_shapes=[pltpu.SemaphoreType.DMA((n_cp,)), pltpu.SemaphoreType.DMA((n_cp,))],
        compiler_params=params(1), name="gather_all",
    )(*w_in, normed, grad_out, normed4, grad4)


def exchange_kernel(o_in, dn_in, a_in, g_in, o_out, dn_out, a_all, g_all, mine, got, parts, res, send, recv):
    me = Place()
    enter(me, [{"c": 1}] + around("x") + around("y") + around("z"))
    cs = Copies(send, recv)
    mate = me.at(c=1)
    swaps = []
    for t, src in enumerate((o_in, dn_in)):
        swaps.append((cs.remote(src.at[1 - me.c], got.at[t], mate), cs.local(src.at[me.c], mine.at[t])))
    rings = []
    for src, buf, axis in ((a_in, a_all, "y"), (g_in, g_all, "z")):
        here = getattr(me, axis)

        def piece(off, h, buf=buf, here=here):
            return buf.at[(here + off + 4) % 4, pl.ds(h * 256, 256)]

        ring = Ring(cs, me, axis, piece, lambda h, src=src: src.at[pl.ds(h * 256, 256)])
        ring.start()
        rings.append((ring, cs.local(src, buf.at[here])))
    sends = []
    for t in range(2):
        swaps[t][0].wait_recv()
        swaps[t][1].wait()
        for k, off in ((2, 2), (0, 1), (1, -1), (3, 0)):
            blk = (me.x + off + 4) % 4

            @pl.loop(0, POS // 16)
            def _(i):
                r = pl.ds(pl.multiple_of(i * 16, 16), 16)
                s = mine[t, blk, r, :].astype(F32) + got[t, blk, r, :].astype(F32)
                mine[t, blk, r, :] = s.astype(BF16)

            if off:
                sends.append(cs.remote(mine.at[t, blk], parts.at[t, k], me.at(x=off)))
    for ring, local in rings:
        ring.forward()
    for t, dst in enumerate((o_out, dn_out)):
        for cp in sends[3 * t:3 * t + 3]:
            cp.wait_recv()

        @pl.loop(0, POS // 16)
        def _(i):
            r = pl.ds(pl.multiple_of(i * 16, 16), 16)
            s = mine[t, me.x, r, :].astype(F32) + parts[t, 0, r, :].astype(F32)
            s = s + parts[t, 1, r, :].astype(F32) + parts[t, 2, r, :].astype(F32)
            dst[r, :] = s.astype(BF16)

    for ring, local in rings:
        ring.near()
        ring.far()
        local.wait()
    cs.drain()


def exchange(o_part, dn_part, attn, grad_qkv):
    ca, cg = attn.shape[1], grad_qkv.shape[1]
    return pl.pallas_call(
        exchange_kernel,
        out_shape=[jax.ShapeDtypeStruct((POS, D), BF16)] * 2
        + [jax.ShapeDtypeStruct((4, 512, ca), BF16), jax.ShapeDtypeStruct((4, 512, cg), BF16)],
        in_specs=[ANY] * 4, out_specs=[VMEM, VMEM, ANY, ANY],
        scratch_shapes=[pltpu.VMEM((2, 4, POS, D), BF16), pltpu.VMEM((2, 4, POS, D), BF16), pltpu.VMEM((2, 3, POS, D), BF16),
                        pltpu.VMEM((8, 128), F32),
                        pltpu.SemaphoreType.DMA((24,)), pltpu.SemaphoreType.DMA((24,))],
        compiler_params=params(2, 60 * 2**20), name="exchange",
    )(o_part, dn_part, attn, grad_qkv)


def scatter_kernel(q_in, o_in, q_out, o_out, send, recv):
    me = Place()
    enter(me, [{axis: k, "c": c} for axis in ("y", "z") for k in (1, -1, 2) for c in (0, 1)] + [{"c": 1}])
    cs = Copies(send, recv)
    waits, locals_ = [], []
    for k, off in ((3, 2), (1, 1), (2, -1), (0, 0)):
        for dc in (0, 1):
            for src, dst, axis in ((q_in, q_out, "y"), (o_in, o_out, "z")):
                blk = (getattr(me, axis) + off + 4) % 4
                core = (me.c + dc) % 2
                piece, slot = src.at[blk, core], dst.at[k, me.c]
                if off or dc:
                    waits.append(cs.remote(piece, slot, me.at(**{axis: off, "c": dc})))
                else:
                    locals_.append(cs.local(piece, slot))
    for cp in waits:
        cp.wait_recv()
    for cp in locals_:
        cp.wait()
    cs.drain()


def scatter(grad_q, grad_o):
    cq, co = grad_q.shape[-1], grad_o.shape[-1]
    return pl.pallas_call(
        scatter_kernel,
        out_shape=[jax.ShapeDtypeStruct((4, 2, HALF, cq), F32), jax.ShapeDtypeStruct((4, 2, HALF, co), F32)],
        in_specs=[ANY] * 2, out_specs=[ANY] * 2,
        scratch_shapes=[pltpu.SemaphoreType.DMA((16,)), pltpu.SemaphoreType.DMA((16,))],
        compiler_params=params(3), name="scatter",
    )(grad_q, grad_o)


def gain_grad_kernel(p_ref, o_ref, rz, ry, rc, rx, sz, sy, sc, sx, send, recv):
    me = Place()
    enter(me, [{"c": 1}] + around("x") + around("y") + around("z"))
    cs = Copies(send, recv)

    def stage(src, slots, axis):
        here = getattr(me, axis)
        offs = [{"c": 1}] if axis == "c" else around(axis)
        n = 2 if axis == "c" else 4
        sent = [cs.remote(src((here + off[axis] + n) % n), slots.at[here], me.at(**off)) for off in offs]
        slots[here] = src(here)[...]
        for cp in sent:
            cp.wait_recv()
        total = slots[0]
        for k in range(1, n):
            total = total + slots[k]
        return total

    sz[...] = stage(lambda k: p_ref.at[k], rz, "z")
    sy[...] = stage(lambda k: sz.at[k], ry, "y")
    sc[...] = stage(lambda k: sy.at[k], rc, "c")
    o_ref[...] = stage(lambda k: sc, rx, "x")
    cs.drain()


def reduce_gain(part):
    padded = jnp.pad(part.reshape(32, HALF), ((0, 0), (0, 1024 - HALF))).reshape(4, 4, 2, 8, 128)
    out = pl.pallas_call(
        gain_grad_kernel,
        out_shape=jax.ShapeDtypeStruct((8, 128), F32),
        in_specs=[VMEM], out_specs=VMEM,
        scratch_shapes=[pltpu.VMEM((4, 4, 2, 8, 128), F32), pltpu.VMEM((4, 2, 8, 128), F32), pltpu.VMEM((2, 8, 128), F32), pltpu.VMEM((4, 8, 128), F32),
                        pltpu.VMEM((4, 2, 8, 128), F32), pltpu.VMEM((2, 8, 128), F32), pltpu.VMEM((8, 128), F32), pltpu.VMEM((8, 128), F32),
                        pltpu.SemaphoreType.DMA((10,)), pltpu.SemaphoreType.DMA((10,))],
        compiler_params=params(4), name="reduce_gain",
    )(padded)
    return out.reshape(1024)[:HALF]


def rope_tables(seq_len):
    half_dim = HEAD_DIM // 2
    inv_freq = ROPE_BASE ** (-jnp.arange(half_dim, dtype=F32) * 2.0 / HEAD_DIM)
    angles = jnp.arange(seq_len, dtype=F32)[:, None] * inv_freq[None, :]
    return jnp.cos(angles), jnp.sin(angles)


def rotate(values, cos_t, sin_t):
    half_dim = values.shape[-1] // 2
    lower_half = values[..., :half_dim]
    upper_half = values[..., half_dim:]
    return jnp.concatenate([lower_half * cos_t - upper_half * sin_t, upper_half * cos_t + lower_half * sin_t], axis=-1)


def dot(spec, a, b):
    return jnp.einsum(spec, a, b, preferred_element_type=F32)


def solution(mesh):
    def local_block(hidden, norm_gain, w_query, w_key, w_value, w_out, grad_out):
        gain_full = gather_gain(norm_gain)
        hidden, grad_out = hidden[0], grad_out[0]
        hidden_f32 = hidden.astype(F32)
        inv_rms = lax.rsqrt(jnp.mean(hidden_f32 * hidden_f32, axis=-1, keepdims=True) + NORM_EPS)
        x_hat = hidden_f32 * inv_rms
        normed = (x_hat * gain_full).astype(BF16)

        w_out_t = w_out.T
        q2 = w_query.reshape(HALF, 2, 896)
        o2 = w_out_t.reshape(HALF, 2, 896)
        k2, v2 = w_key.reshape(HALF, 2, 128), w_value.reshape(HALF, 2, 128)
        w_in = [q2[:, :, :640], jnp.concatenate([q2[:, :, 640:], k2, v2], -1), o2[:, :, :384], o2[:, :, 384:]]
        w_in = [jnp.moveaxis(w, 1, 0) for w in w_in]
        n4 = jnp.moveaxis(normed.reshape(POS, 4, DZ), 1, 0)
        dy4 = jnp.moveaxis(grad_out.reshape(POS, 4, 4, BLK), 2, 0).reshape(4, POS, DZ)
        *w_all, n_all, dy_all, n4_all, dy4_all = gather_all(w_in, normed, grad_out, n4, dy4)
        w0, w1, w2, w3 = [w.reshape(D, -1) for w in w_all]
        n_all, dy_all = n_all.reshape(512, D), dy_all.reshape(512, D)
        n4_all, dy4_all = n4_all.reshape(2048, DZ), dy4_all.reshape(2048, DZ)

        cos_t, sin_t = rope_tables(SEQ)
        cos_q, sin_q = cos_t[:, None, :], sin_t[:, None, :]
        qa = dot("td,de->te", n_all, w0).astype(BF16)
        qb = dot("td,de->te", n_all, w1).astype(BF16)
        q_lin = jnp.concatenate([qa, qb[:, :256]], -1).reshape(2, SEQ, 7, HEAD_DIM)
        k_lin, v_heads = qb[:, 256:384].reshape(2, SEQ, HEAD_DIM), qb[:, 384:].reshape(2, SEQ, HEAD_DIM)
        q_heads = rotate(q_lin.astype(F32), cos_q, sin_q).astype(BF16)
        k_heads = rotate(k_lin.astype(F32), cos_t, sin_t).astype(BF16)
        causal = jnp.arange(SEQ)[:, None] >= jnp.arange(SEQ)[None, :]
        scores = dot("bqrd,bkd->brqk", q_heads, k_heads) * SCORE_SCALE
        attn_prob = jax.nn.softmax(jnp.where(causal, scores, MASK_VALUE), axis=-1)
        prob_bf16 = attn_prob.astype(BF16)
        attn = dot("brqk,bkd->bqrd", prob_bf16, v_heads).astype(BF16).reshape(512, 896)
        o_part = (dot("te,de->td", attn[:, :384], w2) + dot("te,de->td", attn[:, 384:], w3)).astype(BF16)

        ga = [dot("td,de->te", dy_all, w).astype(BF16) for w in (w2, w3)]
        grad_attn = jnp.concatenate(ga, -1).reshape(2, SEQ, 7, HEAD_DIM)
        grad_v = dot("brqk,bqrd->bkd", prob_bf16, grad_attn).astype(BF16)
        grad_prob = dot("bqrd,bkd->brqk", grad_attn, v_heads)
        grad_scores = attn_prob * (grad_prob - jnp.sum(grad_prob * attn_prob, axis=-1, keepdims=True))
        grad_scores = (grad_scores * SCORE_SCALE).astype(BF16)
        grad_q = dot("brqk,bkd->bqrd", grad_scores, k_heads).astype(BF16)
        grad_k = dot("brqk,bqrd->bkd", grad_scores, q_heads).astype(BF16)
        gq = rotate(grad_q.astype(F32), cos_q, -sin_q).astype(BF16).reshape(512, 896)
        gk = rotate(grad_k.astype(F32), cos_t, -sin_t).astype(BF16).reshape(512, 128)
        gqkv = jnp.concatenate([gq, gk, grad_v.reshape(512, 128)], -1)
        dn_part = (dot("te,de->td", gqkv[:, :640], w0) + dot("te,de->td", gqkv[:, 640:], w1)).astype(BF16)

        o_sum, dn_sum, attn_all, gqkv_all = exchange(o_part.reshape(2, 4, POS, D), dn_part.reshape(2, 4, POS, D), attn, gqkv)
        hidden_out = (hidden_f32 + o_sum.astype(F32)).astype(BF16)
        grad_normed = dn_sum.astype(F32)
        value_a9 = grad_normed * gain_full
        grad_hidden = (grad_out.astype(F32) + inv_rms * (value_a9 - x_hat * jnp.mean(value_a9 * x_hat, axis=-1, keepdims=True))).astype(BF16)
        grad_gain = reduce_gain(jnp.sum(grad_normed * x_hat, axis=0))

        gw = dot("td,te->de", n4_all, gqkv_all.reshape(2048, 1152)).reshape(4, 2, HALF, 1152)
        gwo = dot("td,te->de", dy4_all, attn_all.reshape(2048, 896)).reshape(4, 2, HALF, 896)
        gw, gwo = scatter(gw, gwo)
        gw, gwo = jnp.sum(gw, 0), jnp.sum(gwo, 0)
        gw = jnp.moveaxis(gw, 0, 1)
        grad_wo = jnp.moveaxis(gwo, 0, 1).reshape(HALF, DZ).T
        return (
            hidden_out[None],
            grad_hidden[None],
            grad_gain,
            gw[:, :, :896].reshape(HALF, DZ),
            gw[:, :, 896:1024].reshape(HALF, 256),
            gw[:, :, 1024:].reshape(HALF, 256),
            grad_wo,
        )

    act_spec = P("dp", "tp", None)
    col_spec = P("dp", "tp")
    row_spec = P("tp", "dp")
    return jax.shard_map(
        local_block,
        mesh=mesh,
        in_specs=(act_spec, P("dp"), col_spec, col_spec, col_spec, row_spec, act_spec),
        out_specs=(act_spec, act_spec, P("dp"), col_spec, col_spec, col_spec, row_spec),
        check_vma=False,
    )
```

```python
import functools

import jax
import jax.numpy as jnp
from jax import lax
from jax.experimental import pallas as pl
from jax.experimental.pallas import tpu as pltpu
from jax.sharding import PartitionSpec as P

HEAD_DIM = 128
NORM_EPS = 1e-5
ROPE_BASE = 500000.0
SCORE_SCALE = HEAD_DIM ** -0.5
MASK_VALUE = -1e30
MESH = pl.DeviceIdType.MESH
ANY = pl.BlockSpec(memory_space=pl.ANY)
VMEM = pl.BlockSpec(memory_space=pltpu.VMEM)
F32, BF16 = jnp.float32, jnp.bfloat16

D = 7168
SEQ = 256
POS = 64
BLK = 448
HALF = 224
DZ = 1792
W_COLS = (640, 512, 384, 512)
Z_FIRST = (True, False, True, False)


class Place:
    def __init__(self):
        self.x = lax.axis_index("tp")
        dp = lax.axis_index("dp")
        self.z, self.y, self.c = dp // 8, (dp // 2) % 4, dp % 2

    def at(self, x=0, y=0, z=0, c=0):
        x, y, z = (self.x + x + 4) % 4, (self.y + y + 4) % 4, (self.z + z + 4) % 4
        return (x, (z * 4 + y) * 2 + (self.c + c) % 2)


def enter(place, offsets):
    barrier = pltpu.get_barrier_semaphore()
    for off in offsets:
        pl.semaphore_signal(barrier, inc=1, device_id=place.at(**off), device_id_type=MESH)
    pl.semaphore_wait(barrier, len(offsets))


def around(axis):
    return [{axis: 1}, {axis: -1}, {axis: 2}]


class Copies:
    def __init__(self, send, recv):
        self.send, self.recv, self.n, self.all = send, recv, 0, []

    def remote(self, src, dst, device):
        cp = pltpu.make_async_remote_copy(src, dst, self.send.at[self.n], self.recv.at[self.n], device_id=device, device_id_type=MESH)
        self.n += 1
        cp.start()
        self.all.append(cp)
        return cp

    def local(self, src, dst):
        cp = pltpu.make_async_copy(src, dst, self.send.at[self.n])
        self.n += 1
        cp.start()
        return cp

    def drain(self):
        for cp in self.all:
            cp.wait_send()


class Ring:
    def __init__(self, copies, place, axis, piece, own=None):
        self.copies, self.piece = copies, piece
        self.right, self.left = place.at(**{axis: 1}), place.at(**{axis: -1})
        self.own = own or (lambda h: piece(0, h))

    def start(self):
        c, p = self.copies, self.piece
        self.r0 = c.remote(self.own(0), p(0, 0), self.right)
        self.l0 = c.remote(self.own(1), p(0, 1), self.left)
        self.r1 = c.remote(self.own(1), p(0, 1), self.right)
        self.l1 = c.remote(self.own(0), p(0, 0), self.left)

    def forward(self):
        c, p = self.copies, self.piece
        self.r0.wait_recv()
        self.r2 = c.remote(p(-1, 0), p(-1, 0), self.right)
        self.l0.wait_recv()
        self.l2 = c.remote(p(1, 1), p(1, 1), self.left)

    def near(self):
        self.r1.wait_recv()
        self.l1.wait_recv()

    def far(self):
        self.r2.wait_recv()
        self.l2.wait_recv()


def params(cid, vmem=None):
    return pltpu.CompilerParams(collective_id=cid, has_side_effects=True, vmem_limit_bytes=vmem)


def gain_kernel(g_ref, o_ref, send, recv):
    me = Place()
    enter(me, [{"c": 1}] + around("y") + around("z"))
    cs = Copies(send, recv)
    o_ref[me.z, me.y, me.c] = g_ref[...]
    cs.remote(g_ref, o_ref.at[me.z, me.y, me.c], me.at(c=1)).wait_recv()
    for cp in [cs.remote(o_ref.at[me.z, me.y], o_ref.at[me.z, me.y], me.at(**off)) for off in around("y")]:
        cp.wait_recv()
    for cp in [cs.remote(o_ref.at[me.z], o_ref.at[me.z], me.at(**off)) for off in around("z")]:
        cp.wait_recv()
    cs.drain()


def gather_gain(norm_gain):
    padded = jnp.pad(norm_gain.astype(F32), (0, 1024 - HALF)).reshape(8, 128)
    out = pl.pallas_call(
        gain_kernel,
        out_shape=jax.ShapeDtypeStruct((4, 4, 2, 8, 128), F32),
        in_specs=[VMEM], out_specs=VMEM,
        scratch_shapes=[pltpu.SemaphoreType.DMA((7,)), pltpu.SemaphoreType.DMA((7,))],
        compiler_params=params(0), name="gather_gain",
    )(padded)
    return out.reshape(32, 1024)[:, :HALF].reshape(D)


def gather_kernel(*refs):
    w_in, (n_in, dy_in, n4_in, dy4_in) = refs[:4], refs[4:8]
    w_all, (n_all, dy_all, n4_all, dy4_all) = refs[8:12], refs[12:16]
    send, recv = refs[16:]
    me = Place()
    enter(me, [{"c": 1}] + around("x") + around("y") + around("z"))
    cs = Copies(send, recv)
    mate = me.at(c=1)

    rows = pl.ds(pl.multiple_of(me.c * HALF, HALF), HALF)
    first = []
    for w, buf in zip(w_in, w_all):
        first.append((cs.remote(w.at[1 - me.c], buf.at[me.z, me.y, rows], mate), cs.local(w.at[me.c], buf.at[me.z, me.y, rows])))

    def x_piece(buf):
        return lambda off, h: buf.at[me.c, (me.x + off + 4) % 4, pl.ds(h * 32, 32)]

    def x_ring(buf, src):
        return Ring(cs, me, "x", x_piece(buf), lambda h: src.at[pl.ds(h * 32, 32)])

    def x4_ring(buf):
        return Ring(cs, me, "x", lambda off, h: buf.at[pl.ds(2 * h, 2), me.c, (me.x + off + 4) % 4])

    acts = []
    for buf, src in ((n_all, n_in), (dy_all, dy_in)):
        ring = x_ring(buf, src)
        ring.start()
        acts.append((ring, cs.local(src, buf.at[me.c, me.x]), buf))
    fours = []
    for buf, src, axis in ((n4_all, n4_in, "z"), (dy4_all, dy4_in, "y")):
        here = getattr(me, axis)
        moves = [cs.remote(src.at[(here + off[axis] + 4) % 4], buf.at[here, me.c, me.x], me.at(**off)) for off in around(axis)]
        fours.append((moves, cs.local(src.at[here], buf.at[here, me.c, me.x]), x4_ring(buf), buf))

    def phase1(buf, z_first):
        if z_first:
            return Ring(cs, me, "z", lambda off, h: buf.at[(me.z + off + 4) % 4, me.y, pl.ds(h * HALF, HALF)])
        return Ring(cs, me, "y", lambda off, h: buf.at[me.z, (me.y + off + 4) % 4, pl.ds(h * HALF, HALF)])

    def phase2(buf, z_first):
        if z_first:
            return Ring(cs, me, "y", lambda off, h: buf.at[pl.ds(2 * h, 2), (me.y + off + 4) % 4])
        return Ring(cs, me, "z", lambda off, h: buf.at[(me.z + off + 4) % 4, pl.ds(2 * h, 2)])

    ones = [phase1(b, f) for b, f in zip(w_all, Z_FIRST)]
    twos = [phase2(b, f) for b, f in zip(w_all, Z_FIRST)]
    for (remote, local), ring in zip(first, ones):
        remote.wait_recv()
        local.wait()
        ring.start()
    for ring in ones:
        ring.forward()
    for one, two in zip(ones[:2], twos[:2]):
        one.near()
        one.far()
        two.start()
    for one, two in zip(ones[2:], twos[2:]):
        one.near()
        one.far()
        two.start()
    for ring, local, buf in acts:
        local.wait()
        ring.forward()
        ring.near()
    for moves, local, ring, buf in fours:
        for cp in moves:
            cp.wait_recv()
        local.wait()
        ring.start()
    tail = []
    for ring, local, buf in acts:
        for k in (0, 1, -1):
            p = buf.at[me.c, (me.x + k + 4) % 4]
            tail.append(cs.remote(p, p, mate))
    for ring in twos[:2]:
        ring.forward()
    for ring, local, buf in acts:
        ring.far()
        p = buf.at[me.c, (me.x + 2) % 4]
        tail.append(cs.remote(p, p, mate))
    for moves, local, ring, buf in fours:
        ring.forward()
        ring.near()
        for k in (0, 1, -1):
            p = buf.at[:, me.c, (me.x + k + 4) % 4]
            tail.append(cs.remote(p, p, mate))
    for ring in twos[2:]:
        ring.forward()
    for moves, local, ring, buf in fours:
        ring.far()
        p = buf.at[:, me.c, (me.x + 2) % 4]
        tail.append(cs.remote(p, p, mate))
    for ring in twos:
        ring.near()
        ring.far()
    for cp in tail:
        cp.wait_recv()
    cs.drain()


def gather_all(w_in, normed, grad_out, normed4, grad4):
    n_cp = 4 * 14 + 2 * 7 + 2 * 10 + 16
    shapes = [jax.ShapeDtypeStruct((4, 4, BLK, cols), BF16) for cols in W_COLS]
    shapes += [jax.ShapeDtypeStruct((2, 4, POS, D), BF16)] * 2
    shapes += [jax.ShapeDtypeStruct((4, 2, 4, POS, DZ), BF16)] * 2
    return pl.pallas_call(
        gather_kernel,
        out_shape=shapes,
        in_specs=[VMEM] * 8, out_specs=[ANY] * 8,
        scratch_shapes=[pltpu.SemaphoreType.DMA((n_cp,)), pltpu.SemaphoreType.DMA((n_cp,))],
        compiler_params=params(1), name="gather_all",
    )(*w_in, normed, grad_out, normed4, grad4)


class Scatter:
    def __init__(self, copies, place, axis, acc, far_buf, near_buf):
        self.copies, self.acc, self.far_buf, self.near_buf = copies, acc, far_buf, near_buf
        here = getattr(place, axis)
        self.blk = {off: (here + off + 4) % 4 for off in (-1, 0, 1, 2)}
        self.right, self.left = place.at(**{axis: 1}), place.at(**{axis: -1})

    def half(self, off, h):
        return self.acc.at[self.blk[off], pl.ds(h * HALF, HALF)]

    def add(self, off, lo, n, *others):
        @pl.loop(0, n // 32)
        def _(i):
            r = pl.multiple_of(i * 32, 32)
            total = self.acc[self.blk[off], pl.ds(lo + r, 32), :]
            for ref in others:
                total = total + ref[pl.ds(r, 32), :]
            self.acc[self.blk[off], pl.ds(lo + r, 32), :] = total

    def start(self):
        c = self.copies
        self.f0 = c.remote(self.half(2, 0), self.far_buf.at[0], self.right)
        self.f1 = c.remote(self.half(2, 1), self.far_buf.at[1], self.left)
        self.n0 = c.remote(self.half(1, 1), self.near_buf.at[0, pl.ds(HALF, HALF)], self.right)
        self.n1 = c.remote(self.half(-1, 0), self.near_buf.at[1, pl.ds(0, HALF)], self.left)

    def mid(self):
        c = self.copies
        self.f0.wait_recv()
        self.add(1, 0, HALF, self.far_buf.at[0])
        self.n2 = c.remote(self.half(1, 0), self.near_buf.at[0, pl.ds(0, HALF)], self.right)
        self.f1.wait_recv()
        self.add(-1, HALF, HALF, self.far_buf.at[1])
        self.n3 = c.remote(self.half(-1, 1), self.near_buf.at[1, pl.ds(HALF, HALF)], self.left)

    def finish(self):
        for cp in (self.n0, self.n1, self.n2, self.n3):
            cp.wait_recv()
        self.add(0, 0, BLK, self.near_buf.at[0], self.near_buf.at[1])


NT = (((1,), (1,)), ((), ()))
TN = (((0,), (0,)), ((), ()))
DB = 896


def back_kernel(g_in, a_in, hid, dy, rms, gain, w0, w1, w2, w3, n4, dy4,
                y_out, dx_out, gg_out, gq_out, gk_out, gv_out, go_out,
                parts, g_all, a_all, acc_q, acc_o, far_q, near_q, far_o, near_o, act, wa, wb, tmp, own, got, pbuf,
                gp, gz, gs, gy, gc, gx,
                send, recv, act_sem, w_sem, tmp_sem, got_sem, p_sem):
    me = Place()
    enter(me, [{"c": 1}] + around("x") + around("y") + around("z"))
    cs = Copies(send, recv)
    mate = me.at(c=1)

    class SlotRing:
        def __init__(self, axis, src, buf):
            self.right, self.left = me.at(**{axis: 1}), me.at(**{axis: -1})
            self.src, self.buf = src, buf

        def start(self):
            s, b = self.src, self.buf
            lo, hi = pl.ds(0, 256), pl.ds(256, 256)
            self.r0 = cs.remote(s.at[lo], b.at[0, lo], self.right)
            self.l0 = cs.remote(s.at[hi], b.at[1, hi], self.left)
            self.r1 = cs.remote(s.at[hi], b.at[0, hi], self.right)
            self.l1 = cs.remote(s.at[lo], b.at[1, lo], self.left)

        def forward(self):
            b = self.buf
            lo, hi = pl.ds(0, 256), pl.ds(256, 256)
            self.r0.wait_recv()
            self.r2 = cs.remote(b.at[0, lo], b.at[2, lo], self.right)
            self.l0.wait_recv()
            self.l2 = cs.remote(b.at[1, hi], b.at[2, hi], self.left)

        def near(self):
            self.r1.wait_recv()
            self.l1.wait_recv()

        def far(self):
            self.r2.wait_recv()
            self.l2.wait_recv()

    ring_g, ring_a = SlotRing("z", g_in, g_all), SlotRing("y", a_in, a_all)
    ring_g.start()
    ring_a.start()

    def head_product(t, src, wl, wr):
        cl, cr = wl.shape[1], wr.shape[1]

        def fetch(j, slot):
            rows = pl.ds(pl.multiple_of(j * DB, DB), DB)
            return (pltpu.make_async_copy(wl.at[rows], wa.at[slot, :, pl.ds(0, cl)], w_sem.at[slot, 0]),
                    pltpu.make_async_copy(wr.at[rows], wb.at[slot, :, pl.ds(0, cr)], w_sem.at[slot, 1]))

        def give(j, slot):
            cols = pl.ds(pl.multiple_of(j * DB, DB), DB)
            return pltpu.make_async_remote_copy(tmp.at[slot, 1 - me.c], got.at[t, :, :, cols], tmp_sem.at[slot], got_sem.at[t, j],
                                                device_id=mate, device_id_type=MESH)

        for cp in fetch(0, 0):
            cp.start()

        @pl.loop(0, D // DB)
        def _(j):
            slot = j % 2
            for cp in fetch(j, slot):
                cp.wait()

            @pl.when(j < D // DB - 1)
            def _():
                for cp in fetch(j + 1, 1 - slot):
                    cp.start()

            @pl.when(j >= 2)
            def _():
                give(j - 2, slot).wait_send()

            res = lax.dot_general(src[:, :cl], wa[slot, :, :cl], NT, preferred_element_type=F32)
            res = res + lax.dot_general(src[:, cl:], wb[slot, :, :cr], NT, preferred_element_type=F32)
            tmp[slot] = res.astype(BF16).reshape(2, 4, POS, DB)
            give(j, slot).start()
            own[t, :, :, pl.ds(pl.multiple_of(j * DB, DB), DB)] = tmp[slot, me.c]

        for j in (D // DB - 2, D // DB - 1):
            give(j, j % 2).wait_send()

    def share(t):
        @pl.loop(0, D // DB)
        def _(j):
            cols = pl.ds(pl.multiple_of(j * DB, DB), DB)
            pltpu.make_async_remote_copy(tmp.at[0, 0], got.at[t, :, :, cols], tmp_sem.at[0], got_sem.at[t, j],
                                         device_id=mate, device_id_type=MESH).wait_recv()

        sends = []
        for k, off in ((2, 2), (0, 1), (1, -1), (3, 0)):
            blk = (me.x + off + 4) % 4

            @pl.loop(0, POS // 16)
            def _(i):
                r = pl.ds(pl.multiple_of(i * 16, 16), 16)
                s = own[t, blk, r, :].astype(F32) + got[t, blk, r, :].astype(F32)
                own[t, blk, r, :] = s.astype(BF16)

            if off:
                sends.append(cs.remote(own.at[t, blk], parts.at[t, k], me.at(x=off)))
        return sends

    def total(t, r):
        cp = pltpu.make_async_copy(parts.at[t, :, r], pbuf, p_sem)
        cp.start()
        cp.wait()
        s = own[t, me.x, r, :].astype(F32) + pbuf[0].astype(F32)
        s = s + pbuf[1].astype(F32) + pbuf[2].astype(F32)
        return s.astype(BF16).astype(F32)

    def row_half(axis, i):
        return (((getattr(me, axis) + 2) % 4) // 2 + i) % 2

    def act_copy(hbm, piece, axis, i):
        cols = pl.ds(pl.multiple_of(row_half(axis, i) * DB, DB), DB)
        return pltpu.make_async_copy(hbm.at[pl.ds(pl.multiple_of(piece * 512, 512), 512), cols], act.at[i], act_sem.at[i])

    pieces = []
    for axis, off, hbm, acc, rhs in (
        ("z", 0, dy4, acc_o, a_in), ("z", -1, dy4, acc_o, a_all.at[0]), ("z", 1, dy4, acc_o, a_all.at[1]),
        ("y", 0, n4, acc_q, g_in), ("z", 2, dy4, acc_o, a_all.at[2]),
        ("y", -1, n4, acc_q, g_all.at[0]), ("y", 1, n4, acc_q, g_all.at[1]), ("y", 2, n4, acc_q, g_all.at[2]),
    ):
        here = me.y if axis == "z" else me.z
        pieces.append(((hbm, (here + off + 4) % 4, axis), acc, rhs, off == 0))

    for i in range(2):
        act_copy(*pieces[0][0], i).start()

    def weight_grad(k):
        where, acc, rhs, first = pieces[k]

        @pl.loop(0, 2)
        def _(i):
            act_copy(*where, i).wait()
            h = row_half(where[2], i)
            res = lax.dot_general(act[i], rhs[...], TN, preferred_element_type=F32).reshape(2, BLK, rhs.shape[1])
            if first:
                acc[pl.ds(2 * h, 2)] = res
            else:
                acc[pl.ds(2 * h, 2)] = acc[pl.ds(2 * h, 2)] + res
            if k + 1 < len(pieces):
                act_copy(*pieces[k + 1][0], i).start()

    scat_q = Scatter(cs, me, "y", acc_q, far_q, near_q)
    scat_o = Scatter(cs, me, "z", acc_o, far_o, near_o)

    head_product(0, g_in, w0, w1)
    ring_a.forward()
    ring_g.forward()
    dn_sends = share(0)
    weight_grad(0)
    ring_a.near()
    weight_grad(1)
    weight_grad(2)
    weight_grad(3)
    ring_a.far()
    weight_grad(4)
    scat_o.start()
    ring_g.near()
    weight_grad(5)
    weight_grad(6)
    ring_g.far()
    weight_grad(7)
    scat_q.start()
    head_product(1, a_in, w2, w3)
    scat_o.mid()
    o_sends = share(1)
    scat_q.mid()

    for cp in dn_sends:
        cp.wait_recv()
    gp[...] = jnp.zeros_like(gp)

    @pl.loop(0, POS // 16)
    def _(i):
        r = pl.ds(pl.multiple_of(i * 16, 16), 16)
        gn = total(0, r)
        x_hat = hid[r, :].astype(F32) * rms[r, :]
        gp[...] += jnp.sum(gn * x_hat, axis=0, keepdims=True)
        v = gn * gain[...]
        m = jnp.mean(v * x_hat, axis=-1, keepdims=True)
        own[0, me.x, r, :] = (dy[r, :].astype(F32) + rms[r, :] * (v - x_hat * m)).astype(BF16)

    dx_copy = cs.local(own.at[0, me.x], dx_out)

    def gain_stage(src, slots, axis):
        here = getattr(me, axis)
        offs = [{"c": 1}] if axis == "c" else around(axis)
        n = 2 if axis == "c" else 4
        sent = [cs.remote(src((here + off[axis] + n) % n), slots.at[here], me.at(**off)) for off in offs]
        slots[here] = src(here)[...]
        for cp in sent:
            cp.wait_recv()
        s = slots[0]
        for k in range(1, n):
            s = s + slots[k]
        return s

    gs[0] = gain_stage(lambda k: gp.at[:, pl.ds(pl.multiple_of(k * DZ, DZ), DZ)], gz, "z")
    gs[1] = gain_stage(lambda k: gs.at[0], gy, "y")
    gs[2] = gain_stage(lambda k: gs.at[1], gc, "c")
    gg_out[...] = gain_stage(lambda k: gs.at[2], gx, "x")

    def hand_out(scat, outs):
        done = []
        lo = 0
        for out, width in outs:
            cols = pl.ds(pl.multiple_of(me.c * width, width), width)
            rows = lambda core: pl.ds(pl.multiple_of(core * HALF, HALF), HALF)
            src = lambda core: scat.acc.at[scat.blk[0], rows(core), pl.ds(lo, width)]
            done.append((cs.remote(src(1 - me.c), out.at[:, cols], mate), cs.local(src(me.c), out.at[:, cols])))
            lo += width
        return done

    scat_o.finish()
    done = hand_out(scat_o, [(go_out, 896)])
    for cp in o_sends:
        cp.wait_recv()

    @pl.loop(0, POS // 16)
    def _(i):
        r = pl.ds(pl.multiple_of(i * 16, 16), 16)
        own[1, me.x, r, :] = (hid[r, :].astype(F32) + total(1, r)).astype(BF16)

    y_copy = cs.local(own.at[1, me.x], y_out)

    scat_q.finish()
    done += hand_out(scat_q, [(gq_out, 896), (gk_out, 128), (gv_out, 128)])
    for remote, local in done:
        remote.wait_recv()
        local.wait()
    dx_copy.wait()
    y_copy.wait()
    cs.drain()


def back(gqkv, attn, hidden, grad_out, inv_rms, gain, w_all, n4_all, dy4_all):
    sem = pltpu.SemaphoreType.DMA
    n_cp = 12 + 6 + 12 + 10 + 8 + 2
    V = pltpu.VMEM
    return pl.pallas_call(
        back_kernel,
        out_shape=[jax.ShapeDtypeStruct((POS, D), BF16), jax.ShapeDtypeStruct((POS, D), BF16), jax.ShapeDtypeStruct((1, DZ), F32),
                   jax.ShapeDtypeStruct((HALF, DZ), F32), jax.ShapeDtypeStruct((HALF, 256), F32), jax.ShapeDtypeStruct((HALF, 256), F32),
                   jax.ShapeDtypeStruct((HALF, DZ), F32), jax.ShapeDtypeStruct((2, 3, POS, D), BF16)],
        in_specs=[VMEM] * 6 + [ANY] * 6, out_specs=[ANY] * 2 + [VMEM] + [ANY] * 5,
        scratch_shapes=[V((3, 512, 1152), BF16), V((3, 512, 896), BF16), V((4, BLK, 1152), F32), V((4, BLK, 896), F32),
                        V((2, HALF, 1152), F32), V((2, BLK, 1152), F32), V((2, HALF, 896), F32), V((2, BLK, 896), F32),
                        V((2, 512, DB), BF16), V((2, DB, 640), BF16), V((2, DB, 512), BF16),
                        V((2, 2, 4, POS, DB), BF16), V((2, 4, POS, D), BF16), V((2, 4, POS, D), BF16), V((3, 16, D), BF16),
                        V((1, D), F32), V((4, 1, DZ), F32), V((3, 1, DZ), F32), V((4, 1, DZ), F32), V((2, 1, DZ), F32), V((4, 1, DZ), F32),
                        sem((n_cp,)), sem((n_cp,)), sem((2,)), sem((2, 2)), sem((2,)), sem((2, 8)), sem],
        compiler_params=params(2, 66_900_000), name="back",
    )(gqkv, attn, hidden, grad_out, inv_rms, gain, *w_all, n4_all, dy4_all)


def rope_tables(seq_len):
    half_dim = HEAD_DIM // 2
    inv_freq = ROPE_BASE ** (-jnp.arange(half_dim, dtype=F32) * 2.0 / HEAD_DIM)
    angles = jnp.arange(seq_len, dtype=F32)[:, None] * inv_freq[None, :]
    return jnp.cos(angles), jnp.sin(angles)


def rotate(values, cos_t, sin_t):
    half_dim = values.shape[-1] // 2
    lower_half = values[..., :half_dim]
    upper_half = values[..., half_dim:]
    return jnp.concatenate([lower_half * cos_t - upper_half * sin_t, upper_half * cos_t + lower_half * sin_t], axis=-1)


def dot(spec, a, b):
    return jnp.einsum(spec, a, b, preferred_element_type=F32)


def solution(mesh):
    def local_block(hidden, norm_gain, w_query, w_key, w_value, w_out, grad_out):
        gain_full = gather_gain(norm_gain)
        hidden, grad_out = hidden[0], grad_out[0]
        hidden_f32 = hidden.astype(F32)
        inv_rms = lax.rsqrt(jnp.mean(hidden_f32 * hidden_f32, axis=-1, keepdims=True) + NORM_EPS)
        x_hat = hidden_f32 * inv_rms
        normed = (x_hat * gain_full).astype(BF16)

        w_out_t = w_out.T
        q2 = w_query.reshape(HALF, 2, 896)
        o2 = w_out_t.reshape(HALF, 2, 896)
        k2, v2 = w_key.reshape(HALF, 2, 128), w_value.reshape(HALF, 2, 128)
        w_in = [q2[:, :, :640], jnp.concatenate([q2[:, :, 640:], k2, v2], -1), o2[:, :, :384], o2[:, :, 384:]]
        w_in = [jnp.moveaxis(w, 1, 0) for w in w_in]
        n4 = jnp.moveaxis(normed.reshape(POS, 4, DZ), 1, 0)
        dy4 = jnp.moveaxis(grad_out.reshape(POS, 4, 4, BLK), 2, 0).reshape(4, POS, DZ)
        *w_all, n_all, dy_all, n4_all, dy4_all = gather_all(w_in, normed, grad_out, n4, dy4)
        w0, w1, w2, w3 = [w.reshape(D, -1) for w in w_all]
        n_all, dy_all = n_all.reshape(512, D), dy_all.reshape(512, D)
        n4_all, dy4_all = n4_all.reshape(2048, DZ), dy4_all.reshape(2048, DZ)

        cos_t, sin_t = rope_tables(SEQ)
        cos_q, sin_q = cos_t[:, None, :], sin_t[:, None, :]
        qa = dot("td,de->te", n_all, w0).astype(BF16)
        qb = dot("td,de->te", n_all, w1).astype(BF16)
        q_lin = jnp.concatenate([qa, qb[:, :256]], -1).reshape(2, SEQ, 7, HEAD_DIM)
        k_lin, v_heads = qb[:, 256:384].reshape(2, SEQ, HEAD_DIM), qb[:, 384:].reshape(2, SEQ, HEAD_DIM)
        q_heads = rotate(q_lin.astype(F32), cos_q, sin_q).astype(BF16)
        k_heads = rotate(k_lin.astype(F32), cos_t, sin_t).astype(BF16)
        causal = jnp.arange(SEQ)[:, None] >= jnp.arange(SEQ)[None, :]
        scores = dot("bqrd,bkd->brqk", q_heads, k_heads) * SCORE_SCALE
        attn_prob = jax.nn.softmax(jnp.where(causal, scores, MASK_VALUE), axis=-1)
        prob_bf16 = attn_prob.astype(BF16)
        attn = dot("brqk,bkd->bqrd", prob_bf16, v_heads).astype(BF16).reshape(512, 896)
        ga = [dot("td,de->te", dy_all, w).astype(BF16) for w in (w2, w3)]
        grad_attn = jnp.concatenate(ga, -1).reshape(2, SEQ, 7, HEAD_DIM)
        grad_v = dot("brqk,bqrd->bkd", prob_bf16, grad_attn).astype(BF16)
        grad_prob = dot("bqrd,bkd->brqk", grad_attn, v_heads).astype(BF16).astype(F32)
        grad_scores = attn_prob * (grad_prob - jnp.sum(grad_prob * attn_prob, axis=-1, keepdims=True))
        grad_scores = (grad_scores * SCORE_SCALE).astype(BF16)
        grad_q = dot("brqk,bkd->bqrd", grad_scores, k_heads).astype(BF16)
        grad_k = dot("brqk,bqrd->bkd", grad_scores, q_heads).astype(BF16)
        gq = rotate(grad_q.astype(F32), cos_q, -sin_q).astype(BF16).reshape(512, 896)
        gk = rotate(grad_k.astype(F32), cos_t, -sin_t).astype(BF16).reshape(512, 128)
        gqkv = jnp.concatenate([gq, gk, grad_v.reshape(512, 128)], -1)
        y, dx, gg, gq, gk, gv, go, _ = back(gqkv, attn, hidden, grad_out, inv_rms, gain_full[None], (w0, w1, w2, w3), n4_all, dy4_all)
        grad_gain = lax.dynamic_slice(gg[0], ((lax.axis_index("dp") % 8) * HALF,), (HALF,))
        return y[None], dx[None], grad_gain, gq, gk, gv, go.T

    act_spec = P("dp", "tp", None)
    col_spec = P("dp", "tp")
    row_spec = P("tp", "dp")
    return jax.shard_map(
        local_block,
        mesh=mesh,
        in_specs=(act_spec, P("dp"), col_spec, col_spec, col_spec, row_spec, act_spec),
        out_specs=(act_spec, act_spec, P("dp"), col_spec, col_spec, col_spec, row_spec),
        check_vma=False,
    )
```
